8 devices in a mesh: depth: 2 (over z, y), col: 2 (over x), row: 2 (over core).
Axes of the slice: x: 2, y: 2, z: 1, core: 2. Of those that a mesh axis runs over, the one named last changes fastest.
Arguments:
- reach_in: bfloat16 [7168, 7168], P(('row', 'depth'), 'col')
Outputs:
- output: bfloat16 [7168, 7168], P(('row', 'depth'), 'col')
All inputs are finite; a program needn't handle non-finite values.
Results may differ from the reference program's by a relative error of at most 0.001.
Values are sent between devices in bfloat16 or wider.
A program may use at most 1 GiB of HBM per device.

```python
import jax
import jax.numpy as jnp
from jax import lax

N = 7168
SQUARINGS = 4


def setup_inputs(seed: int = 0) -> dict:
    root_key = jax.random.key(seed)
    position = jax.random.permutation(root_key, N)
    chain_edges = position[None, :] == position[:, None] + 1
    return {'reach_in': chain_edges.astype(jnp.float32).astype(jnp.bfloat16)}


def reference(reach_in):
    def square_once(current, unused_x):
        path_count = jnp.dot(current, current, preferred_element_type=jnp.float32)
        next_reach = jnp.minimum(path_count + current.astype(jnp.float32), 1.0).astype(jnp.bfloat16)
        return next_reach, None
    final_reach, unused_ys = lax.scan(square_once, reach_in, None, length=SQUARINGS)
    return final_reach
```

```python
import functools

import jax
import jax.numpy as jnp
from jax import lax
from jax.experimental import pallas as pl
from jax.experimental.pallas import tpu as pltpu
from jax.sharding import PartitionSpec as P

SQUARINGS = 4
UNIT = 128
TILE_N = 512
MESH = pl.DeviceIdType.MESH
OWN, PARTNER, VERT, PARTNER_VERT, HORI = range(5)


def chunk_plan(quarter):
    units = quarter // UNIT
    widths = [2] * (units // 2 - 1) + [1, 1]
    plan = []
    start = 0
    local_start = 0
    for c, w in enumerate(widths):
        if c == len(widths) - 1:
            lw = 0
        else:
            lw = 2
        plan.append((start * UNIT, w * UNIT, local_start * UNIT, lw * UNIT))
        start += w
        local_start += lw
    assert start == units and local_start == units
    return plan


def kernel(plan, in_ref, out_ref, work, acc, a_buf, b_buf, stage, x_send, x_recv, y_send, y_recv, p_send, p_recv, r_send,
           r_recv, a_sem, b_sem, o_sem):
    depth = lax.axis_index('depth')
    col = lax.axis_index('col')
    row = lax.axis_index('row')
    rows, cols = in_ref.shape
    quarter = cols // 2
    tiles = cols // TILE_N
    n_chunks = len(plan)
    x_dev = {'col': 1 - col}
    y_dev = {'depth': 1 - depth}
    p_dev = {'row': 1 - row}
    differ = lax.rem(row + col, 2)
    near = pl.multiple_of(depth * quarter, UNIT)
    far = pl.multiple_of((1 - depth) * quarter, UNIT)

    barrier = pltpu.get_barrier_semaphore()
    for dev in (x_dev, y_dev, p_dev):
        pl.semaphore_signal(barrier, inc=1, device_id=dev, device_id_type=MESH)
    pl.semaphore_wait(barrier, 3)

    def remote(src, dst, s_sem, r_sem, dev):
        return pltpu.make_async_remote_copy(src_ref=src, dst_ref=dst, send_sem=s_sem, recv_sem=r_sem, device_id=dev,
                                            device_id_type=MESH)

    def sends(source, par, c):
        start, width, lstart, lwidth = plan[c]
        piece = source.at[pl.ds(start, width), :]
        out = [remote(piece, work.at[par, VERT, pl.ds(start, width), :], y_send.at[par, c], y_recv.at[par, c], y_dev)]
        for h, base in enumerate((near, far)):
            where = pl.ds(pl.multiple_of(base + start, UNIT), width)
            out.append(remote(source.at[:, where], work.at[par, HORI, :, where], x_send.at[par, c, h],
                              x_recv.at[par, c, h], x_dev))
        if lwidth:
            local = pl.ds(lstart, lwidth)
            out.append(remote(source.at[local, :], work.at[par, PARTNER, local, :], p_send.at[par, c],
                              p_recv.at[par, c], p_dev))
        return out

    def relay(par, c):
        start, width, _, _ = plan[c]
        return remote(work.at[par, VERT, pl.ds(start, width), :], work.at[par, PARTNER_VERT, pl.ds(start, width), :],
                      r_send.at[par, c], r_recv.at[par, c], p_dev)

    def start_all(source, par):
        for c in range(n_chunks):
            for copy in sends(source, par, c):
                copy.start()

    start_all(in_ref, 0)

    @pl.loop(0, tiles)
    def _(n):
        where = pl.ds(pl.multiple_of(n * TILE_N, TILE_N), TILE_N)
        load = pltpu.make_async_copy(in_ref.at[:, where], stage.at[0], o_sem.at[0])
        load.start()
        load.wait()
        acc[n] = stage[0].astype(jnp.float32)
        store = pltpu.make_async_copy(stage.at[0], work.at[0, OWN, :, where], o_sem.at[0])
        store.start()
        store.wait()

    def squaring(t, carry):
        par = lax.rem(t, 2)

        @pl.when(t > 0)
        def _():
            start_all(work.at[par, OWN], par)

        for c in range(n_chunks):
            start, width, lstart, lwidth = plan[c]
            last = c == n_chunks - 1
            own_sends = sends(work.at[par, OWN], par, c)
            for copy in own_sends[1:] + own_sends[:1]:
                copy.wait_recv()
            pass_on = relay(par, c)
            pass_on.start()
            pass_on.wait_recv()
            pieces = []
            if lwidth:
                pieces.append((OWN, near, lstart, lwidth, OWN + differ))
            pieces.append((OWN, far, start, width, VERT + differ))
            pieces.append((HORI, near, start, width, PARTNER - differ))
            pieces.append((HORI, far, start, width, PARTNER_VERT - differ))
            offset = 0
            loads = []
            for k, (a_slot, base, s, w, b_slot) in enumerate(pieces):
                where = pl.ds(pl.multiple_of(base + s, UNIT), w)
                loads.append(pltpu.make_async_copy(work.at[par, a_slot, :, where], a_buf.at[:, pl.ds(offset, w)],
                                                   a_sem.at[k]))
                loads.append(pltpu.make_async_copy(work.at[par, b_slot, pl.ds(s, w), :], b_buf.at[pl.ds(offset, w), :],
                                                   b_sem.at[k]))
                offset += w
            for copy in loads:
                copy.start()
            for copy in loads:
                copy.wait()
            width_k = offset

            if not last:
                @pl.loop(0, tiles)
                def _(n):
                    where = pl.ds(pl.multiple_of(n * TILE_N, TILE_N), TILE_N)
                    acc[n] += jnp.dot(a_buf[:, :width_k], b_buf[:width_k, where], preferred_element_type=jnp.float32)
            else:
                def store(n, slot, dst):
                    where = pl.ds(pl.multiple_of(n * TILE_N, TILE_N), TILE_N)
                    return pltpu.make_async_copy(stage.at[slot], dst.at[:, where], o_sem.at[slot])

                def finish(n, carry):
                    where = pl.ds(pl.multiple_of(n * TILE_N, TILE_N), TILE_N)
                    slot = lax.rem(n, 2)

                    @pl.when(n >= 2)
                    def _():
                        store(n, slot, out_ref).wait()

                    product = jnp.dot(a_buf[:, :width_k], b_buf[:width_k, where], preferred_element_type=jnp.float32)
                    fresh = jnp.minimum(acc[n] + product, 1.0)
                    acc[n] = fresh
                    stage[slot] = fresh.astype(jnp.bfloat16)

                    @pl.when(t == SQUARINGS - 1)
                    def _():
                        store(n, slot, out_ref).start()

                    @pl.when(t < SQUARINGS - 1)
                    def _():
                        store(n, slot, work.at[1 - par, OWN]).start()

                    return carry

                lax.fori_loop(0, tiles, finish, 0)
                for n in (tiles - 2, tiles - 1):
                    store(n, n % 2, out_ref).wait()

        for c in range(n_chunks):
            for copy in sends(work.at[par, OWN], par, c):
                copy.wait_send()
            relay(par, c).wait_send()
        return carry

    lax.fori_loop(0, SQUARINGS, squaring, 0)


def solution(mesh):
    def run(slab):
        rows, cols = slab.shape
        plan = chunk_plan(cols // 2)
        n_chunks = len(plan)
        k_max = max(3 * w + lw for _, w, _, lw in plan)
        dma = pltpu.SemaphoreType.DMA
        out, _ = pl.pallas_call(
            functools.partial(kernel, plan),
            out_shape=(jax.ShapeDtypeStruct((rows, cols), jnp.bfloat16),
                       jax.ShapeDtypeStruct((2, 5, rows, cols), jnp.bfloat16)),
            in_specs=[pl.BlockSpec(memory_space=pl.ANY)],
            out_specs=(pl.BlockSpec(memory_space=pl.ANY), pl.BlockSpec(memory_space=pl.ANY)),
            scratch_shapes=[
                pltpu.VMEM((cols // TILE_N, rows, TILE_N), jnp.float32),
                pltpu.VMEM((rows, k_max), jnp.bfloat16),
                pltpu.VMEM((k_max, cols), jnp.bfloat16),
                pltpu.VMEM((2, rows, TILE_N), jnp.bfloat16),
                dma((2, n_chunks, 2)), dma((2, n_chunks, 2)),
                dma((2, n_chunks)), dma((2, n_chunks)),
                dma((2, n_chunks)), dma((2, n_chunks)),
                dma((2, n_chunks)), dma((2, n_chunks)),
                dma((4,)), dma((4,)), dma((2,)),
            ],
            compiler_params=pltpu.CompilerParams(collective_id=0, has_side_effects=True,
                                                 vmem_limit_bytes=67_000_000),
            name='reach_squarings',
        )(slab)
        return out

    layout = P(('row', 'depth'), 'col')
    return jax.shard_map(run, mesh=mesh, in_specs=(layout,), out_specs=layout, check_vma=False)
```

```python
import functools

import jax
import jax.numpy as jnp
from jax import lax
from jax.experimental import pallas as pl
from jax.experimental.pallas import tpu as pltpu
from jax.sharding import PartitionSpec as P

SQUARINGS = 4
SUB = 256
TILE = 512
BLOCK = 448
RING = 3
MESH = pl.DeviceIdType.MESH
OWN, MATE, VERT, MATE_VERT, HORI, MATE_HORI, DIAG, MATE_DIAG = range(8)
LEFT_O = (OWN, HORI)
LEFT_Y = (VERT, DIAG)


class Place:
    def __init__(self, half):
        self.depth = lax.axis_index('depth')
        self.col = lax.axis_index('col')
        self.row = lax.axis_index('row')
        self.differ = lax.rem(self.row + self.col, 2)
        self.half = half
        self.per = half // SUB

    def base(self, f):
        return pl.multiple_of((self.depth + f - 2 * self.depth * f) * self.half, SUB)

    def cols(self, r):
        f, q = r // self.per, r % self.per
        return pl.ds(pl.multiple_of((self.depth + f - 2 * self.depth * f) * self.half + q * SUB, SUB), SUB)

    def rows(self, q):
        return pl.ds(pl.multiple_of(q * SUB, SUB), SUB)

    def right_slot(self, base, h, f):
        return base + 2 * f + (self.differ if h == 0 else 1 - self.differ)


class Engine:
    def __init__(self, place, a_buf, b_buf, acc, ring, eye, a_sem, b_sem, out_sem):
        self.place, self.a_buf, self.b_buf, self.acc, self.ring, self.eye = place, a_buf, b_buf, acc, ring, eye
        self.a_sem, self.b_sem, self.out_sem = a_sem, b_sem, out_sem
        down = lax.broadcasted_iota(jnp.int32, eye.shape, 0)
        across = lax.broadcasted_iota(jnp.int32, eye.shape, 1)
        eye[...] = (down == across).astype(jnp.float32).astype(jnp.bfloat16)

    def load(self, src, slot, lefts, rights, tile0, nt, full):
        p = self.place
        for e in range(2):
            a_slot, r = lefts[e]
            pltpu.make_async_copy(src.at[a_slot, :, p.cols(r)], self.a_buf.at[slot, :, pl.ds(e * SUB, SUB)],
                                  self.a_sem.at[slot]).start()
            b_slot, q = rights[e]
            if full:
                for f, width in enumerate((p.half, nt * TILE - p.half)):
                    pltpu.make_async_copy(src.at[b_slot, p.rows(q), pl.ds(p.base(f), width)],
                                          self.b_buf.at[slot, pl.ds(e * SUB, SUB), pl.ds(f * p.half, width)],
                                          self.b_sem.at[slot]).start()
            else:
                for g in range(2 * nt):
                    pltpu.make_async_copy(src.at[b_slot, p.rows(q), p.cols(2 * tile0 + g)],
                                          self.b_buf.at[slot, pl.ds(e * SUB, SUB), pl.ds(g * SUB, SUB)],
                                          self.b_sem.at[slot]).start()

    def ready(self, src, slot, tile0, nt, ones):
        k = 2 * SUB
        pltpu.make_async_copy(src.at[0, :, pl.ds(0, k)], self.a_buf.at[slot], self.a_sem.at[slot]).wait()
        pltpu.make_async_copy(src.at[0, pl.ds(0, k), pl.ds(0, nt * TILE)],
                              self.b_buf.at[slot, :, pl.ds(0, nt * TILE)], self.b_sem.at[slot]).wait()
        for e, r in ones:
            @pl.when((r >= 2 * tile0) & (r < 2 * (tile0 + nt)))
            def _():
                where = pl.ds(pl.multiple_of((r - 2 * tile0) * SUB, SUB), SUB)
                self.b_buf[slot, e * SUB:(e + 1) * SUB, where] += self.eye[...]

    def product(self, slot, t, rows):
        where = pl.ds(pl.multiple_of(t * TILE, TILE), TILE)
        return jnp.dot(self.a_buf[slot, rows, :], self.b_buf[slot, :, where], preferred_element_type=jnp.float32)

    def step(self, slot, which, tile0, nt, init):
        blocks = [pl.ds(m, BLOCK) for m in range(0, self.a_buf.shape[1], BLOCK)]

        def add(t):
            for rows in blocks:
                before = self.acc[which, tile0 + t, rows, :]
                if init is not False:
                    before = jnp.where(init, 0.0, before)
                self.acc[which, tile0 + t, rows, :] = before + self.product(slot, t, rows)

        if nt > 1:
            @pl.loop(0, nt // 2)
            def _(g):
                add(2 * g)
                add(2 * g + 1)
        if nt % 2:
            add(nt - 1)

    def finish(self, slot, which, tile0, nt, dst, before, after):
        p = self.place
        ring_size, part = self.ring.shape[0], self.ring.shape[1]
        parts = self.a_buf.shape[1] // part

        def put(u):
            t, h, s = u // parts, u % parts, u % ring_size
            rows = pl.ds(pl.multiple_of(h * part, part), part)
            return [pltpu.make_async_copy(self.ring.at[s, :, pl.ds(e * SUB, SUB)],
                                          dst.at[rows, p.cols(2 * (tile0 + t) + e)], self.out_sem.at[s, e])
                    for e in range(2)]

        def put_wait(u):
            for c in put(u):
                c.wait()

            @pl.when(u % parts == parts - 1)
            def _():
                after(tile0 + u // parts)

        n = nt * parts
        before()

        def body(u, carry):
            s = lax.rem(u, ring_size)

            @pl.when(u >= ring_size)
            def _():
                put_wait(u - ring_size)

            t = u // parts
            base = (u % parts) * part
            for m in range(0, part, BLOCK):
                rows = pl.ds(pl.multiple_of(base + m, BLOCK), BLOCK)
                total = self.acc[which, tile0 + t, rows, :] + self.product(slot, t, rows)
                self.ring[s, m:m + BLOCK, :] = jnp.minimum(total, 1.0).astype(jnp.bfloat16)
            for c in put(u):
                c.start()
            return carry

        lax.fori_loop(0, n, body, 0)

        def tail(u, carry):
            put_wait(u)
            return carry

        lax.fori_loop(max(0, n - ring_size), n, tail, 0)

    def gemm(self, src, n, load, which, tile0, nt, first, ones, final=None):
        load(0, 0)

        def body(k, carry):
            slot = lax.rem(k, 2)

            @pl.when(k + 1 < n)
            def _():
                load(k + 1, 1 - slot)

            self.ready(src, slot, tile0, nt, ones(k))
            self.step(slot, which, tile0, nt, (k == 0) if first else False)
            return carry

        lax.fori_loop(0, n - 1 if final else n, body, 0)
        if final:
            slot = (n - 1) % 2
            dst, after = final
            self.finish(slot, which, tile0, nt, dst, lambda: self.ready(src, slot, tile0, nt, ones(n - 1)), after)


def nothing(*args):
    return None


def square_tiles(engine, src, tile0, nt, full, final, arrive=nothing):
    p = engine.place

    def load(k, slot):
        arrive(k)
        f, q = k // p.per, k % p.per
        engine.load(src, slot, [(OWN, k), (HORI, k)],
                    [(p.right_slot(0, 0, f), q), (p.right_slot(0, 1, f), q)], tile0, nt, full)

    engine.gemm(src, 2 * p.per, load, 0, tile0, nt, True, lambda k: [(0, k)], final)


def pair_kernel(in_ref, new, work, acc, a_buf, b_buf, ring, eye, a_sem, b_sem, out_sem, x_s, x_r, y_s, y_r, m_s, m_r, mx_s,
                mx_r, my_s, my_r, dx_s, dx_r, dy_s, dy_r, md_s, md_r, n_s, n_r, ny_s, ny_r,
                ex_s, ex_r, ey_s, ey_r):
    rows, cols = in_ref.shape
    p = Place(cols // 2)
    per, half = p.per, p.half
    count = 2 * per
    tiles = cols // TILE
    kept = tiles - 1
    top = pl.ds(0, rows // 2)
    low = pl.ds(rows // 2, rows // 2)
    x_dev = {'col': 1 - p.col}
    y_dev = {'depth': 1 - p.depth}
    m_dev = {'row': 1 - p.row}
    engine = Engine(p, a_buf, b_buf, acc, ring, eye, a_sem, b_sem, out_sem)

    barrier = pltpu.get_barrier_semaphore()
    for dev in (x_dev, y_dev, m_dev):
        pl.semaphore_signal(barrier, inc=1, device_id=dev, device_id_type=MESH)
    pl.semaphore_wait(barrier, 3)

    def remote(src, dst, s_sem, r_sem, dev):
        return pltpu.make_async_remote_copy(src_ref=src, dst_ref=dst, send_sem=s_sem, recv_sem=r_sem, device_id=dev,
                                            device_id_type=MESH)

    def send_x(src, s, r):
        return remote(src.at[:, p.cols(r)], work.at[s, HORI, :, p.cols(r)], x_s.at[r], x_r.at[r], x_dev)

    def send_mate(src, s, r):
        return remote(src.at[:, p.cols(r)], work.at[s, MATE, :, p.cols(r)], m_s.at[r], m_r.at[r], m_dev)

    def send_y_near(src, s, q):
        return remote(src.at[:, p.cols(q)], work.at[s, VERT, :, p.cols(q)], y_s.at[q], y_r.at[q], y_dev)

    def send_y_far(src, s, q):
        far = pl.ds(p.base(1), half)
        return remote(src.at[p.rows(q), far], work.at[s, VERT, p.rows(q), far], y_s.at[per + q], y_r.at[per + q], y_dev)

    def pass_x(s, r):
        return remote(work.at[s, HORI, :, p.cols(r)], work.at[s, MATE_HORI, :, p.cols(r)], mx_s.at[r], mx_r.at[r], m_dev)

    def pass_y_near(s, q):
        return remote(work.at[s, VERT, :, p.cols(per + q)], work.at[s, MATE_VERT, :, p.cols(per + q)], my_s.at[q],
                      my_r.at[q], m_dev)

    def pass_y_far(s, q):
        near = pl.ds(p.base(0), half)
        return remote(work.at[s, VERT, p.rows(q), near], work.at[s, MATE_VERT, p.rows(q), near], my_s.at[per + q],
                      my_r.at[per + q], m_dev)

    def pass_diag(s, r):
        return remote(work.at[s, DIAG, :, p.cols(r)], work.at[s, MATE_DIAG, :, p.cols(r)], md_s.at[r], md_r.at[r], m_dev)

    def forward_x(s, r):
        return remote(work.at[s, VERT, top, p.cols(r)], work.at[s, DIAG, top, p.cols(r)], dx_s.at[r], dx_r.at[r], x_dev)

    def forward_y(s, r):
        mine = p.cols(lax.rem(r + per, count))
        return remote(work.at[s, HORI, low, mine], work.at[s, DIAG, low, mine], dy_s.at[r], dy_r.at[r], y_dev)

    def send_new(t):
        return remote(new.at[OWN], new.at[MATE], n_s.at[0], n_r.at[0], m_dev)

    def send_new_y(r):
        return remote(new.at[VERT, :, p.cols(r)], new.at[MATE_VERT, :, p.cols(r)], ny_s.at[r], ny_r.at[r], m_dev)

    def edge_x(e):
        where = p.cols(2 * kept + e)
        return remote(new.at[OWN, :, where], new.at[HORI, :, where], ex_s.at[e], ex_r.at[e], x_dev)

    def edge_y(e):
        where = p.cols(2 * kept + e - per)
        return remote(new.at[OWN, :, where], new.at[VERT, :, where], ey_s.at[e], ey_r.at[e], y_dev)

    def exchange(s, carry):
        src = work.at[s]

        @pl.when(s == 0)
        def _():
            for r in range(count):
                send_x(in_ref, 0, r).start()
                if r < per:
                    send_y_near(in_ref, 0, r).start()
                else:
                    send_y_far(in_ref, 0, r - per).start()
                send_mate(in_ref, 0, r).start()

            @pl.loop(0, tiles)
            def _(t):
                where = pl.ds(pl.multiple_of(t * TILE, TILE), TILE)
                for h, part in enumerate((top, low)):
                    load = pltpu.make_async_copy(in_ref.at[part, where], ring.at[h], out_sem.at[h, 0])
                    load.start()
                    load.wait()
                    store = pltpu.make_async_copy(ring.at[h], work.at[0, OWN, part, where], out_sem.at[h, 0])
                    store.start()
                    store.wait()

        @pl.loop(0, count)
        def _(r):
            send_mate(work.at[s, OWN], s, r).wait_recv()

        def own_load(f, q, slot):
            engine.load(src, slot, [(OWN, f * per + q), (HORI, f * per + q)],
                        [(p.right_slot(0, 0, f), q), (p.right_slot(0, 1, f), q)], 0, tiles, True)

        def near_arrive(q, slot):
            send_x(work.at[s, OWN], s, q).wait_recv()
            pass_x(s, q).start()
            own_load(0, q, slot)
            send_y_near(work.at[s, OWN], s, q).wait_recv()
            pass_y_near(s, q).start()
            pass_x(s, q).wait_recv()
            pass_y_near(s, q).wait_recv()

        engine.gemm(src, per, near_arrive, 0, 0, tiles, True, lambda k: [(0, k)])

        def hori(tile0, nt, f, final):
            def load(k, slot):
                engine.load(src, slot, [(OWN, f * per + k), (HORI, f * per + k)],
                            [(p.right_slot(HORI, 0, f), k), (p.right_slot(HORI, 1, f), k)], tile0, nt, False)

            engine.gemm(src, per, load, 1, tile0, nt, f == 0, lambda k: [(1, f * per + k)], final)

        hori_final = (new.at[HORI], nothing)

        def far_arrive(q):
            send_x(work.at[s, OWN], s, per + q).wait_recv()
            pass_x(s, per + q).start()
            forward_y(s, q).start()
            send_y_far(work.at[s, OWN], s, q).wait_recv()
            pass_y_far(s, q).start()

        def far_half(q, carry):
            far_arrive(q)

            @pl.when(q == per // 2)
            def _():
                @pl.loop(0, per)
                def _(r):
                    forward_x(s, r).start()

            pass_x(s, per + q).wait_recv()
            pass_y_far(s, q).wait_recv()
            own_load(1, q, 0)
            engine.ready(src, 0, 0, tiles, [(0, per + q)])
            engine.step(0, 0, 0, tiles, False)

            @pl.when(lax.rem(q, 2) == 0)
            def _():
                hori(q, 2, 0, None)

            return carry

        lax.fori_loop(0, per - 1, far_half, 0)
        far_arrive(per - 1)

        @pl.loop(per, count)
        def _(r):
            forward_x(s, r).start()
            forward_y(s, r).start()

        pass_x(s, count - 1).wait_recv()
        pass_y_far(s, per - 1).wait_recv()
        own_load(1, per - 1, 0)
        engine.finish(0, 0, 0, tiles, new.at[OWN], lambda: engine.ready(src, 0, 0, tiles, [(0, count - 1)]), nothing)
        send_new(0).start()
        for e in range(2):
            edge_x(e).start()
            edge_y(e).start()

        def vert_home(k, slot):
            engine.load(src, slot, [(VERT, k), (VERT, per + k)], [(p.right_slot(0, 0, 0), k), (p.right_slot(0, 0, 1), k)],
                        0, kept, True)

        engine.gemm(src, per, vert_home, 0, 0, kept, True, lambda k: [(0, k), (1, per + k)])

        def vert_away(first):
            def load(k, slot):
                r = first + 2 * k
                engine.load(src, slot, [(DIAG, r), (DIAG, r + 1)],
                            [(p.right_slot(0, 1, r // per), r % per), (p.right_slot(0, 1, (r + 1) // per), (r + 1) % per)],
                            0, kept, True)

            return load

        def diag_arrive(r, carry):
            forward_x(s, r).wait_recv()
            forward_y(s, r).wait_recv()

            @pl.when(r < 2 * kept)
            def _():
                pass_diag(s, r).start()

            return carry

        def diag_mate(r, carry):
            pass_diag(s, r).wait_recv()
            return carry

        def diag_group(g, carry):
            first = 4 * g
            lax.fori_loop(first, first + 4, diag_arrive, 0)
            engine.gemm(src, 2, vert_away(first), 0, 0, kept, False, lambda k: [])
            lax.fori_loop(first, first + 4, diag_mate, 0)
            hori(2 * g, 2, 1, hori_final)
            return carry

        lax.fori_loop(0, per // 2, diag_group, 0)
        lax.fori_loop(count - 2, count, diag_arrive, 0)
        vert_away(count - 2)(0, 0)

        def new_y(t):
            for e in range(2):
                send_new_y(2 * t + e).start()

        engine.finish(0, 0, 0, kept, new.at[VERT], lambda: engine.ready(src, 0, 0, kept, []), new_y)
        send_new(0).wait_recv()

        def drain(r, carry):
            own = work.at[s, OWN]
            for copy in (send_x(own, s, r), send_mate(own, s, r), pass_x(s, r), forward_x(s, r), forward_y(s, r)):
                copy.wait_send()

            @pl.when(r < 2 * kept)
            def _():
                pass_diag(s, r).wait_send()

            @pl.when(r < per)
            def _():
                send_y_near(own, s, r).wait_send()
                send_y_far(own, s, r).wait_send()
                pass_y_near(s, r).wait_send()
                pass_y_far(s, r).wait_send()

            return carry

        lax.fori_loop(0, count, drain, 0)

        def new_y_arrive():
            def body(r, carry):
                send_new_y(r).wait_recv()
                return carry

            lax.fori_loop(0, count, body, 0)
            for e in range(2):
                edge_x(e).wait_recv()

        def all_sent():
            send_new(0).wait_send()
            for e in range(2):
                edge_x(e).wait_send()
                edge_y(e).wait_send()

            def sent(r, carry):
                send_new_y(r).wait_send()
                return carry

            lax.fori_loop(0, count, sent, 0)

        for e in range(2):
            edge_y(e).wait_recv()
            send_new_y(2 * kept + e).start()

        @pl.when(s == 0)
        def _():
            fresh = work.at[1, OWN]

            def go(t):
                for e in range(2):
                    r = 2 * t + e
                    send_x(fresh, 1, r).start()
                    send_mate(fresh, 1, r).start()

                    @pl.when(r < per)
                    def _():
                        send_y_near(fresh, 1, r).start()

            def arrive(k):
                if isinstance(k, int):
                    return

                @pl.when(k == per)
                def _():
                    new_y_arrive()

            square_tiles(engine, new, 0, 1, False, (fresh, go), arrive)

            def group(g, carry):
                square_tiles(engine, new, 1 + 2 * g, 2, False, (fresh, go))
                return carry

            lax.fori_loop(0, tiles // 2, group, 0)
            all_sent()
            for q in range(per):
                send_y_far(fresh, 1, q).start()

        @pl.when(s > 0)
        def _():
            new_y_arrive()
            all_sent()

        return carry

    lax.fori_loop(0, SQUARINGS // 2, exchange, 0)


def last_kernel(new, out_ref, acc, a_buf, b_buf, ring, eye, a_sem, b_sem, out_sem):
    cols = out_ref.shape[1]
    p = Place(cols // 2)
    engine = Engine(p, a_buf, b_buf, acc, ring, eye, a_sem, b_sem, out_sem)
    square_tiles(engine, new, 0, cols // TILE, True, (out_ref, nothing))


def solution(mesh):
    def run(slab):
        rows, cols = slab.shape
        count = cols // SUB
        tiles = cols // TILE
        dma = pltpu.SemaphoreType.DMA
        hbm = pl.BlockSpec(memory_space=pl.ANY)

        def scratch(n_acc):
            return [
                pltpu.VMEM((n_acc, tiles, rows, TILE), jnp.float32),
                pltpu.VMEM((2, rows, 2 * SUB), jnp.bfloat16),
                pltpu.VMEM((2, 2 * SUB, cols), jnp.bfloat16),
                pltpu.VMEM((RING, rows // 2, TILE), jnp.bfloat16),
                pltpu.VMEM((SUB, SUB), jnp.bfloat16),
                dma((2,)), dma((2,)), dma((RING, 2)),
            ]

        new, _ = pl.pallas_call(
            pair_kernel,
            out_shape=(jax.ShapeDtypeStruct((5, rows, cols), jnp.bfloat16),
                       jax.ShapeDtypeStruct((2, 8, rows, cols), jnp.bfloat16)),
            in_specs=[hbm],
            out_specs=(hbm, hbm),
            scratch_shapes=scratch(2) + [dma((count,)) for _ in range(16)] + [dma((1,)), dma((1,)), dma((count,)),
                                                                              dma((count,))] + [dma((2,))] * 4,
            compiler_params=pltpu.CompilerParams(collective_id=0, has_side_effects=True, vmem_limit_bytes=67_000_000),
            name='reach_pairs',
        )(slab)
        return pl.pallas_call(
            last_kernel,
            out_shape=jax.ShapeDtypeStruct((rows, cols), jnp.bfloat16),
            in_specs=[hbm],
            out_specs=hbm,
            scratch_shapes=scratch(1),
            compiler_params=pltpu.CompilerParams(vmem_limit_bytes=67_000_000),
            name='reach_last',
        )(new)

    layout = P(('row', 'depth'), 'col')
    return jax.shard_map(run, mesh=mesh, in_specs=(layout,), out_specs=layout, check_vma=False)
```

```python
import functools

import jax
import jax.numpy as jnp
from jax import lax
from jax.experimental import pallas as pl
from jax.experimental.pallas import tpu as pltpu
from jax.sharding import PartitionSpec as P

SQUARINGS = 4
SUB = 256
TILE = 512
BLOCK = 224
RING = 3
MESH = pl.DeviceIdType.MESH
OWN, MATE, VERT, MATE_VERT, HORI, MATE_HORI, DIAG, MATE_DIAG = range(8)
LEFT_O = (OWN, HORI)
LEFT_Y = (VERT, DIAG)


class Place:
    def __init__(self, half):
        self.depth = lax.axis_index('depth')
        self.col = lax.axis_index('col')
        self.row = lax.axis_index('row')
        self.differ = lax.rem(self.row + self.col, 2)
        self.half = half
        self.per = half // SUB

    def base(self, f):
        return pl.multiple_of((self.depth + f - 2 * self.depth * f) * self.half, SUB)

    def cols(self, r):
        f, q = r // self.per, r % self.per
        return pl.ds(pl.multiple_of((self.depth + f - 2 * self.depth * f) * self.half + q * SUB, SUB), SUB)

    def rows(self, q):
        return pl.ds(pl.multiple_of(q * SUB, SUB), SUB)

    def right_slot(self, base, h, f):
        return base + 2 * f + (self.differ if h == 0 else 1 - self.differ)


class Engine:
    def __init__(self, place, a_buf, b_buf, acc, ring, eye, a_sem, b_sem, out_sem):
        self.place, self.a_buf, self.b_buf, self.acc, self.ring, self.eye = place, a_buf, b_buf, acc, ring, eye
        self.a_sem, self.b_sem, self.out_sem = a_sem, b_sem, out_sem
        down = lax.broadcasted_iota(jnp.int32, eye.shape, 0)
        across = lax.broadcasted_iota(jnp.int32, eye.shape, 1)
        eye[...] = (down == across).astype(jnp.float32).astype(jnp.bfloat16)

    def load(self, src, slot, lefts, rights, tile0, nt, full):
        p = self.place
        for e in range(2):
            a_slot, r = lefts[e]
            pltpu.make_async_copy(src.at[a_slot, :, p.cols(r)], self.a_buf.at[slot, :, pl.ds(e * SUB, SUB)],
                                  self.a_sem.at[slot]).start()
            b_slot, q = rights[e]
            if full:
                for f, width in enumerate((p.half, nt * TILE - p.half)):
                    pltpu.make_async_copy(src.at[b_slot, p.rows(q), pl.ds(p.base(f), width)],
                                          self.b_buf.at[slot, pl.ds(e * SUB, SUB), pl.ds(f * p.half, width)],
                                          self.b_sem.at[slot]).start()
            else:
                for g in range(2 * nt):
                    pltpu.make_async_copy(src.at[b_slot, p.rows(q), p.cols(2 * tile0 + g)],
                                          self.b_buf.at[slot, pl.ds(e * SUB, SUB), pl.ds(g * SUB, SUB)],
                                          self.b_sem.at[slot]).start()

    def ready(self, src, slot, tile0, nt, ones):
        k = 2 * SUB
        pltpu.make_async_copy(src.at[0, :, pl.ds(0, k)], self.a_buf.at[slot], self.a_sem.at[slot]).wait()
        pltpu.make_async_copy(src.at[0, pl.ds(0, k), pl.ds(0, nt * TILE)],
                              self.b_buf.at[slot, :, pl.ds(0, nt * TILE)], self.b_sem.at[slot]).wait()
        for e, r in ones:
            @pl.when((r >= 2 * tile0) & (r < 2 * (tile0 + nt)))
            def _():
                where = pl.ds(pl.multiple_of((r - 2 * tile0) * SUB, SUB), SUB)
                self.b_buf[slot, e * SUB:(e + 1) * SUB, where] += self.eye[...]

    def product(self, slot, t, rows):
        where = pl.ds(pl.multiple_of(t * TILE, TILE), TILE)
        return jnp.dot(self.a_buf[slot, rows, :], self.b_buf[slot, :, where], preferred_element_type=jnp.float32)

    def step(self, slot, which, tile0, nt, init):
        blocks = [pl.ds(m, BLOCK) for m in range(0, self.a_buf.shape[1], BLOCK)]

        def add(t):
            for rows in blocks:
                before = self.acc[which, tile0 + t, rows, :]
                if init is not False:
                    before = jnp.where(init, 0.0, before)
                self.acc[which, tile0 + t, rows, :] = before + self.product(slot, t, rows)

        if nt > 1:
            @pl.loop(0, nt // 2)
            def _(g):
                add(2 * g)
                add(2 * g + 1)
        if nt % 2:
            add(nt - 1)

    def finish(self, slot, which, tile0, nt, dst, before, after):
        p = self.place
        ring_size, part = self.ring.shape[0], self.ring.shape[1]
        parts = self.a_buf.shape[1] // part

        def put(u):
            t, h, s = u // parts, u % parts, u % ring_size
            rows = pl.ds(pl.multiple_of(h * part, part), part)
            return [pltpu.make_async_copy(self.ring.at[s, :, pl.ds(e * SUB, SUB)],
                                          dst.at[rows, p.cols(2 * (tile0 + t) + e)], self.out_sem.at[s, e])
                    for e in range(2)]

        def put_wait(u):
            for c in put(u):
                c.wait()

            @pl.when(u % parts == parts - 1)
            def _():
                after(tile0 + u // parts)

        n = nt * parts
        before()

        def body(u, carry):
            s = lax.rem(u, ring_size)

            @pl.when(u >= ring_size)
            def _():
                put_wait(u - ring_size)

            t = u // parts
            base = (u % parts) * part
            for m in range(0, part, BLOCK):
                rows = pl.ds(pl.multiple_of(base + m, BLOCK), BLOCK)
                total = self.acc[which, tile0 + t, rows, :] + self.product(slot, t, rows)
                self.ring[s, m:m + BLOCK, :] = jnp.minimum(total, 1.0).astype(jnp.bfloat16)
            for c in put(u):
                c.start()
            return carry

        lax.fori_loop(0, n, body, 0)

        def tail(u, carry):
            put_wait(u)
            return carry

        lax.fori_loop(max(0, n - ring_size), n, tail, 0)

    def gemm(self, src, n, load, which, tile0, nt, first, ones, final=None, start=0, loaded=False, following=None):
        if not loaded:
            load(0, start)

        def body(k, carry):
            slot = (start + k) % 2

            @pl.when(k + 1 < n)
            def _():
                load(k + 1, 1 - slot)

            if following and not final:
                @pl.when(k + 1 == n)
                def _():
                    following(1 - slot)

            self.ready(src, slot, tile0, nt, ones(k))
            self.step(slot, which, tile0, nt, (k == 0) if first else False)
            return carry

        lax.fori_loop(0, n - 1 if final else n, body, 0)
        if final:
            slot = (start + n - 1) % 2
            dst, after = final

            def before():
                if following:
                    following(1 - slot)
                self.ready(src, slot, tile0, nt, ones(n - 1))

            self.finish(slot, which, tile0, nt, dst, before, after)


def nothing(*args):
    return None


def square_load(engine, src, k, slot, tile0, nt, full):
    p = engine.place
    f, q = k // p.per, k % p.per
    engine.load(src, slot, [(OWN, k), (HORI, k)], [(p.right_slot(0, 0, f), q), (p.right_slot(0, 1, f), q)], tile0, nt, full)


def square_tiles(engine, src, tile0, nt, full, final, arrive=nothing, **chain):
    def load(k, slot):
        arrive(k)
        square_load(engine, src, k, slot, tile0, nt, full)

    engine.gemm(src, 2 * engine.place.per, load, 0, tile0, nt, True, lambda k: [(0, k)], final, **chain)


def pair_kernel(in_ref, new, work, acc, a_buf, b_buf, ring, eye, a_sem, b_sem, out_sem, x_s, x_r, y_s, y_r, m_s, m_r, mx_s,
                mx_r, my_s, my_r, dx_s, dx_r, dy_s, dy_r, md_s, md_r, n_s, n_r, ny_s, ny_r,
                ex_s, ex_r, ey_s, ey_r):
    rows, cols = in_ref.shape
    p = Place(cols // 2)
    per, half = p.per, p.half
    count = 2 * per
    tiles = cols // TILE
    kept = tiles - 1
    top = pl.ds(0, rows // 2)
    low = pl.ds(rows // 2, rows // 2)
    x_dev = {'col': 1 - p.col}
    y_dev = {'depth': 1 - p.depth}
    m_dev = {'row': 1 - p.row}
    engine = Engine(p, a_buf, b_buf, acc, ring, eye, a_sem, b_sem, out_sem)

    barrier = pltpu.get_barrier_semaphore()
    for dev in (x_dev, y_dev, m_dev):
        pl.semaphore_signal(barrier, inc=1, device_id=dev, device_id_type=MESH)
    pl.semaphore_wait(barrier, 3)

    def remote(src, dst, s_sem, r_sem, dev):
        return pltpu.make_async_remote_copy(src_ref=src, dst_ref=dst, send_sem=s_sem, recv_sem=r_sem, device_id=dev,
                                            device_id_type=MESH)

    def send_x(src, s, r):
        return remote(src.at[:, p.cols(r)], work.at[s, HORI, :, p.cols(r)], x_s.at[r], x_r.at[r], x_dev)

    def send_mate(src, s, r):
        return remote(src.at[:, p.cols(r)], work.at[s, MATE, :, p.cols(r)], m_s.at[r], m_r.at[r], m_dev)

    def send_y_near(src, s, q):
        return remote(src.at[:, p.cols(q)], work.at[s, VERT, :, p.cols(q)], y_s.at[q], y_r.at[q], y_dev)

    def send_y_far(src, s, q):
        far = pl.ds(p.base(1), half)
        return remote(src.at[p.rows(q), far], work.at[s, VERT, p.rows(q), far], y_s.at[per + q], y_r.at[per + q], y_dev)

    def pass_x(s, r):
        return remote(work.at[s, HORI, :, p.cols(r)], work.at[s, MATE_HORI, :, p.cols(r)], mx_s.at[r], mx_r.at[r], m_dev)

    def pass_y_near(s, q):
        return remote(work.at[s, VERT, :, p.cols(per + q)], work.at[s, MATE_VERT, :, p.cols(per + q)], my_s.at[q],
                      my_r.at[q], m_dev)

    def pass_y_far(s, q):
        near = pl.ds(p.base(0), half)
        return remote(work.at[s, VERT, p.rows(q), near], work.at[s, MATE_VERT, p.rows(q), near], my_s.at[per + q],
                      my_r.at[per + q], m_dev)

    def pass_diag(s, r):
        return remote(work.at[s, DIAG, :, p.cols(r)], work.at[s, MATE_DIAG, :, p.cols(r)], md_s.at[r], md_r.at[r], m_dev)

    def forward_x(s, r):
        return remote(work.at[s, VERT, top, p.cols(r)], work.at[s, DIAG, top, p.cols(r)], dx_s.at[r], dx_r.at[r], x_dev)

    def forward_y(s, r):
        mine = p.cols(lax.rem(r + per, count))
        return remote(work.at[s, HORI, low, mine], work.at[s, DIAG, low, mine], dy_s.at[r], dy_r.at[r], y_dev)

    def send_new(t):
        return remote(new.at[OWN], new.at[MATE], n_s.at[0], n_r.at[0], m_dev)

    def send_new_y(r):
        return remote(new.at[VERT, :, p.cols(r)], new.at[MATE_VERT, :, p.cols(r)], ny_s.at[r], ny_r.at[r], m_dev)

    def edge_x(e):
        where = p.cols(2 * kept + e)
        return remote(new.at[OWN, :, where], new.at[HORI, :, where], ex_s.at[e], ex_r.at[e], x_dev)

    def edge_y(e):
        where = p.cols(2 * kept + e - per)
        return remote(new.at[OWN, :, where], new.at[VERT, :, where], ey_s.at[e], ey_r.at[e], y_dev)

    def exchange(s, carry):
        src = work.at[s]

        @pl.when(s == 0)
        def _():
            for r in range(count):
                send_x(in_ref, 0, r).start()
                if r < per:
                    send_y_near(in_ref, 0, r).start()
                else:
                    send_y_far(in_ref, 0, r - per).start()
                send_mate(in_ref, 0, r).start()

            @pl.loop(0, tiles)
            def _(t):
                where = pl.ds(pl.multiple_of(t * TILE, TILE), TILE)
                for h, part in enumerate((top, low)):
                    load = pltpu.make_async_copy(in_ref.at[part, where], ring.at[h], out_sem.at[h, 0])
                    load.start()
                    load.wait()
                    store = pltpu.make_async_copy(ring.at[h], work.at[0, OWN, part, where], out_sem.at[h, 0])
                    store.start()
                    store.wait()

        @pl.loop(0, count)
        def _(r):
            send_mate(work.at[s, OWN], s, r).wait_recv()

        def own_load(f, q, slot):
            engine.load(src, slot, [(OWN, f * per + q), (HORI, f * per + q)],
                        [(p.right_slot(0, 0, f), q), (p.right_slot(0, 1, f), q)], 0, tiles, True)

        def near_arrive(q, slot):
            send_x(work.at[s, OWN], s, q).wait_recv()
            pass_x(s, q).start()
            own_load(0, q, slot)
            send_y_near(work.at[s, OWN], s, q).wait_recv()
            pass_y_near(s, q).start()
            pass_x(s, q).wait_recv()
            pass_y_near(s, q).wait_recv()

        def hori(tile0, nt, f, final, start, following, loaded=True):
            engine.gemm(src, per, hori_load(tile0, nt, f), 1, tile0, nt, f == 0, lambda k: [(1, f * per + k)], final,
                        start, loaded, following)

        def hori_load(tile0, nt, f):
            def load(k, slot):
                engine.load(src, slot, [(OWN, f * per + k), (HORI, f * per + k)],
                            [(p.right_slot(HORI, 0, f), k), (p.right_slot(HORI, 1, f), k)], tile0, nt, False)

            return load

        hori_final = (new.at[HORI], nothing)

        def far_prepare(q, slot):
            send_x(work.at[s, OWN], s, per + q).wait_recv()
            pass_x(s, per + q).start()
            forward_y(s, q).start()
            send_y_far(work.at[s, OWN], s, q).wait_recv()
            pass_y_far(s, q).start()

            @pl.when(q == per // 2)
            def _():
                @pl.loop(0, per)
                def _(r):
                    forward_x(s, r).start()

            @pl.when(q == per - 1)
            def _():
                @pl.loop(per, count)
                def _(r):
                    forward_x(s, r).start()
                    forward_y(s, r).start()

            pass_x(s, per + q).wait_recv()
            pass_y_far(s, q).wait_recv()
            own_load(1, q, slot)

        engine.gemm(src, per, near_arrive, 0, 0, tiles, True, lambda k: [(0, k)],
                    following=lambda slot: far_prepare(jnp.int32(0), slot))

        def far_half(q, carry):
            slot = 1 - (q // 2) % 2
            even = lax.rem(q, 2) == 0

            @pl.when(even)
            def _():
                hori_load(q, 2, 0)(0, 1 - slot)

            @pl.when(jnp.logical_not(even))
            def _():
                far_prepare(q + 1, 1 - slot)

            engine.ready(src, slot, 0, tiles, [(0, per + q)])
            engine.step(slot, 0, 0, tiles, False)

            @pl.when(even)
            def _():
                hori(q, 2, 0, None, 1 - slot, lambda after: far_prepare(q + 1, after))

            return carry

        lax.fori_loop(0, per - 1, far_half, 0)
        last = 1 - ((per - 1) // 2) % 2

        def own_before():
            vert_home(0, 1 - last)
            engine.ready(src, last, 0, tiles, [(0, count - 1)])

        def vert_home(k, slot):
            engine.load(src, slot, [(VERT, k), (VERT, per + k)], [(p.right_slot(0, 0, 0), k), (p.right_slot(0, 0, 1), k)],
                        0, kept, True)

        engine.finish(last, 0, 0, tiles, new.at[OWN], own_before, nothing)
        send_new(0).start()
        for e in range(2):
            edge_x(e).start()
            edge_y(e).start()

        def vert_away(first):
            def load(k, slot):
                r = first + 2 * k
                engine.load(src, slot, [(DIAG, r), (DIAG, r + 1)],
                            [(p.right_slot(0, 1, r // per), r % per), (p.right_slot(0, 1, (r + 1) // per), (r + 1) % per)],
                            0, kept, True)

            return load

        def diag_arrive(r, carry):
            forward_x(s, r).wait_recv()
            forward_y(s, r).wait_recv()

            @pl.when(r < 2 * kept)
            def _():
                pass_diag(s, r).start()

            return carry

        def diag_mate(r, carry):
            pass_diag(s, r).wait_recv()
            return carry

        def diag_next(first, slot):
            lax.fori_loop(first, jnp.minimum(first + 4, count), diag_arrive, 0)
            vert_away(first)(0, slot)

        engine.gemm(src, per, vert_home, 0, 0, kept, True, lambda k: [(0, k), (1, per + k)], None, 1 - last, True,
                    lambda slot: diag_next(jnp.int32(0), slot))

        def diag_group(g, carry):
            first = 4 * g
            slot = (last + g) % 2

            def mate_next(after):
                lax.fori_loop(first, first + 4, diag_mate, 0)
                hori_load(2 * g, 2, 1)(0, after)

            engine.gemm(src, 2, vert_away(first), 0, 0, kept, False, lambda k: [], None, slot, True, mate_next)
            hori(2 * g, 2, 1, hori_final, slot, lambda after: diag_next(first + 4, after))
            return carry

        lax.fori_loop(0, per // 2, diag_group, 0)

        def new_y(t):
            for e in range(2):
                send_new_y(2 * t + e).start()

        ending = (last + per // 2) % 2
        engine.finish(ending, 0, 0, kept, new.at[VERT], lambda: engine.ready(src, ending, 0, kept, []), new_y)
        send_new(0).wait_recv()

        def drain(r, carry):
            own = work.at[s, OWN]
            for copy in (send_x(own, s, r), send_mate(own, s, r), pass_x(s, r), forward_x(s, r), forward_y(s, r)):
                copy.wait_send()

            @pl.when(r < 2 * kept)
            def _():
                pass_diag(s, r).wait_send()

            @pl.when(r < per)
            def _():
                send_y_near(own, s, r).wait_send()
                send_y_far(own, s, r).wait_send()
                pass_y_near(s, r).wait_send()
                pass_y_far(s, r).wait_send()

            return carry

        lax.fori_loop(0, count, drain, 0)

        def new_y_arrive():
            def body(r, carry):
                send_new_y(r).wait_recv()
                return carry

            lax.fori_loop(0, count, body, 0)
            for e in range(2):
                edge_x(e).wait_recv()

        def all_sent():
            send_new(0).wait_send()
            for e in range(2):
                edge_x(e).wait_send()
                edge_y(e).wait_send()

            def sent(r, carry):
                send_new_y(r).wait_send()
                return carry

            lax.fori_loop(0, count, sent, 0)

        for e in range(2):
            edge_y(e).wait_recv()
            send_new_y(2 * kept + e).start()

        @pl.when(s == 0)
        def _():
            fresh = work.at[1, OWN]

            def go(t):
                for e in range(2):
                    r = 2 * t + e
                    send_x(fresh, 1, r).start()
                    send_mate(fresh, 1, r).start()

                    @pl.when(r < per)
                    def _():
                        send_y_near(fresh, 1, r).start()

            def arrive(k):
                if isinstance(k, int):
                    return

                @pl.when(k == per)
                def _():
                    new_y_arrive()

            square_tiles(engine, new, 0, 1, False, (fresh, go), arrive,
                         following=lambda slot: square_load(engine, new, 0, slot, 1, 2, False))

            def group(g, carry):
                def following(slot):
                    @pl.when(g + 1 < tiles // 2)
                    def _():
                        square_load(engine, new, 0, slot, 3 + 2 * g, 2, False)

                square_tiles(engine, new, 1 + 2 * g, 2, False, (fresh, go), loaded=True, following=following)
                return carry

            lax.fori_loop(0, tiles // 2, group, 0)
            all_sent()
            for q in range(per):
                send_y_far(fresh, 1, q).start()

        @pl.when(s > 0)
        def _():
            new_y_arrive()
            all_sent()

        return carry

    lax.fori_loop(0, SQUARINGS // 2, exchange, 0)


def last_kernel(new, out_ref, acc, a_buf, b_buf, ring, eye, a_sem, b_sem, out_sem):
    cols = out_ref.shape[1]
    p = Place(cols // 2)
    engine = Engine(p, a_buf, b_buf, acc, ring, eye, a_sem, b_sem, out_sem)
    square_tiles(engine, new, 0, cols // TILE, True, (out_ref, nothing))


def solution(mesh):
    def run(slab):
        rows, cols = slab.shape
        count = cols // SUB
        tiles = cols // TILE
        dma = pltpu.SemaphoreType.DMA
        hbm = pl.BlockSpec(memory_space=pl.ANY)

        def scratch(n_acc):
            return [
                pltpu.VMEM((n_acc, tiles, rows, TILE), jnp.float32),
                pltpu.VMEM((2, rows, 2 * SUB), jnp.bfloat16),
                pltpu.VMEM((2, 2 * SUB, cols), jnp.bfloat16),
                pltpu.VMEM((RING, rows // 2, TILE), jnp.bfloat16),
                pltpu.VMEM((SUB, SUB), jnp.bfloat16),
                dma((2,)), dma((2,)), dma((RING, 2)),
            ]

        new, _ = pl.pallas_call(
            pair_kernel,
            out_shape=(jax.ShapeDtypeStruct((5, rows, cols), jnp.bfloat16),
                       jax.ShapeDtypeStruct((2, 8, rows, cols), jnp.bfloat16)),
            in_specs=[hbm],
            out_specs=(hbm, hbm),
            scratch_shapes=scratch(2) + [dma((count,)) for _ in range(16)] + [dma((1,)), dma((1,)), dma((count,)),
                                                                              dma((count,))] + [dma((2,))] * 4,
            compiler_params=pltpu.CompilerParams(collective_id=0, has_side_effects=True, vmem_limit_bytes=67_000_000),
            name='reach_pairs',
        )(slab)
        return pl.pallas_call(
            last_kernel,
            out_shape=jax.ShapeDtypeStruct((rows, cols), jnp.bfloat16),
            in_specs=[hbm],
            out_specs=hbm,
            scratch_shapes=scratch(1),
            compiler_params=pltpu.CompilerParams(vmem_limit_bytes=67_000_000),
            name='reach_last',
        )(new)

    layout = P(('row', 'depth'), 'col')
    return jax.shard_map(run, mesh=mesh, in_specs=(layout,), out_specs=layout, check_vma=False)
```

```python
import functools

import jax
import jax.numpy as jnp
from jax import lax
from jax.experimental import pallas as pl
from jax.experimental.pallas import tpu as pltpu
from jax.sharding import PartitionSpec as P

SQUARINGS = 4
SUB = 256
TILE = 512
BLOCK = 224
RING = 3
MESH = pl.DeviceIdType.MESH
OWN, MATE, VERT, MATE_VERT, HORI, MATE_HORI, DIAG, MATE_DIAG = range(8)
LEFT_O = (OWN, HORI)
LEFT_Y = (VERT, DIAG)


class Place:
    def __init__(self, half):
        self.depth = lax.axis_index('depth')
        self.col = lax.axis_index('col')
        self.row = lax.axis_index('row')
        self.differ = lax.rem(self.row + self.col, 2)
        self.half = half
        self.per = half // SUB

    def base(self, f):
        return pl.multiple_of((self.depth + f - 2 * self.depth * f) * self.half, SUB)

    def cols(self, r):
        f, q = r // self.per, r % self.per
        return pl.ds(pl.multiple_of((self.depth + f - 2 * self.depth * f) * self.half + q * SUB, SUB), SUB)

    def rows(self, q):
        return pl.ds(pl.multiple_of(q * SUB, SUB), SUB)

    def right_slot(self, base, h, f):
        return base + 2 * f + (self.differ if h == 0 else 1 - self.differ)


class Engine:
    def __init__(self, place, a_buf, b_buf, acc, ring, eye, a_sem, b_sem, out_sem):
        self.place, self.a_buf, self.b_buf, self.acc, self.ring, self.eye = place, a_buf, b_buf, acc, ring, eye
        self.a_sem, self.b_sem, self.out_sem = a_sem, b_sem, out_sem
        down = lax.broadcasted_iota(jnp.int32, eye.shape, 0)
        across = lax.broadcasted_iota(jnp.int32, eye.shape, 1)
        eye[...] = (down == across).astype(jnp.float32).astype(jnp.bfloat16)

    def load(self, src, slot, lefts, rights, tile0, nt, full):
        p = self.place
        for e in range(2):
            a_slot, r = lefts[e]
            pltpu.make_async_copy(src.at[a_slot, :, p.cols(r)], self.a_buf.at[slot, :, pl.ds(e * SUB, SUB)],
                                  self.a_sem.at[slot]).start()
            b_slot, q = rights[e]
            if full:
                for f, width in enumerate((p.half, nt * TILE - p.half)):
                    pltpu.make_async_copy(src.at[b_slot, p.rows(q), pl.ds(p.base(f), width)],
                                          self.b_buf.at[slot, pl.ds(e * SUB, SUB), pl.ds(f * p.half, width)],
                                          self.b_sem.at[slot]).start()
            else:
                for g in range(2 * nt):
                    pltpu.make_async_copy(src.at[b_slot, p.rows(q), p.cols(2 * tile0 + g)],
                                          self.b_buf.at[slot, pl.ds(e * SUB, SUB), pl.ds(g * SUB, SUB)],
                                          self.b_sem.at[slot]).start()

    def ready(self, src, slot, tile0, nt, ones):
        k = 2 * SUB
        pltpu.make_async_copy(src.at[0, :, pl.ds(0, k)], self.a_buf.at[slot], self.a_sem.at[slot]).wait()
        pltpu.make_async_copy(src.at[0, pl.ds(0, k), pl.ds(0, nt * TILE)],
                              self.b_buf.at[slot, :, pl.ds(0, nt * TILE)], self.b_sem.at[slot]).wait()
        for e, r in ones:
            @pl.when((r >= 2 * tile0) & (r < 2 * (tile0 + nt)))
            def _():
                where = pl.ds(pl.multiple_of((r - 2 * tile0) * SUB, SUB), SUB)
                self.b_buf[slot, e * SUB:(e + 1) * SUB, where] += self.eye[...]

    def product(self, slot, t, rows):
        where = pl.ds(pl.multiple_of(t * TILE, TILE), TILE)
        return jnp.dot(self.a_buf[slot, rows, :], self.b_buf[slot, :, where], preferred_element_type=jnp.float32)

    def step(self, slot, which, tile0, nt, init, unrolled=False):
        blocks = [pl.ds(m, BLOCK) for m in range(0, self.a_buf.shape[1], BLOCK)]

        def add(t):
            for rows in blocks:
                before = self.acc[which, tile0 + t, rows, :]
                if init is not False:
                    before = jnp.where(init, 0.0, before)
                self.acc[which, tile0 + t, rows, :] = before + self.product(slot, t, rows)

        if unrolled:
            for t in range(nt):
                add(t)
            return
        if nt > 1:
            @pl.loop(0, nt // 2)
            def _(g):
                add(2 * g)
                add(2 * g + 1)
        if nt % 2:
            add(nt - 1)

    def finish(self, slot, which, tile0, nt, dst, before, after):
        p = self.place
        ring_size, part = self.ring.shape[0], self.ring.shape[1]
        parts = self.a_buf.shape[1] // part

        def put(u):
            t, h, s = u // parts, u % parts, u % ring_size
            rows = pl.ds(pl.multiple_of(h * part, part), part)
            return [pltpu.make_async_copy(self.ring.at[s, :, pl.ds(e * SUB, SUB)],
                                          dst.at[rows, p.cols(2 * (tile0 + t) + e)], self.out_sem.at[s, e])
                    for e in range(2)]

        def put_wait(u):
            for c in put(u):
                c.wait()

            @pl.when(u % parts == parts - 1)
            def _():
                after(tile0 + u // parts)

        n = nt * parts
        before()

        def body(u, carry):
            s = lax.rem(u, ring_size)

            @pl.when(u >= ring_size)
            def _():
                put_wait(u - ring_size)

            t = u // parts
            base = (u % parts) * part
            for m in range(0, part, BLOCK):
                rows = pl.ds(pl.multiple_of(base + m, BLOCK), BLOCK)
                total = self.acc[which, tile0 + t, rows, :] + self.product(slot, t, rows)
                self.ring[s, m:m + BLOCK, :] = jnp.minimum(total, 1.0).astype(jnp.bfloat16)
            for c in put(u):
                c.start()
            return carry

        lax.fori_loop(0, n, body, 0)

        def tail(u, carry):
            put_wait(u)
            return carry

        lax.fori_loop(max(0, n - ring_size), n, tail, 0)

    def gemm(self, src, n, load, which, tile0, nt, first, ones, final=None, start=0, loaded=False, following=None,
             unrolled=False):
        if not loaded:
            load(0, start)

        def body(k, carry):
            slot = (start + k) % 2

            @pl.when(k + 1 < n)
            def _():
                load(k + 1, 1 - slot)

            if following and not final:
                @pl.when(k + 1 == n)
                def _():
                    following(1 - slot)

            self.ready(src, slot, tile0, nt, ones(k))
            self.step(slot, which, tile0, nt, (k == 0) if first else False, unrolled)
            return carry

        lax.fori_loop(0, n - 1 if final else n, body, 0)
        if final:
            slot = (start + n - 1) % 2
            dst, after = final

            def before():
                if following:
                    following(1 - slot)
                self.ready(src, slot, tile0, nt, ones(n - 1))

            self.finish(slot, which, tile0, nt, dst, before, after)


def nothing(*args):
    return None


def square_load(engine, src, k, slot, tile0, nt, full):
    p = engine.place
    f, q = k // p.per, k % p.per
    engine.load(src, slot, [(OWN, k), (HORI, k)], [(p.right_slot(0, 0, f), q), (p.right_slot(0, 1, f), q)], tile0, nt, full)


def square_tiles(engine, src, tile0, nt, full, final, arrive=nothing, **chain):
    def load(k, slot):
        arrive(k)
        square_load(engine, src, k, slot, tile0, nt, full)

    engine.gemm(src, 2 * engine.place.per, load, 0, tile0, nt, True, lambda k: [(0, k)], final, unrolled=full, **chain)


def pair_kernel(in_ref, new, work, acc, a_buf, b_buf, ring, eye, a_sem, b_sem, out_sem, x_s, x_r, y_s, y_r, m_s, m_r, mx_s,
                mx_r, my_s, my_r, dx_s, dx_r, dy_s, dy_r, md_s, md_r, n_s, n_r, ny_s, ny_r,
                ex_s, ex_r, ey_s, ey_r):
    rows, cols = in_ref.shape
    p = Place(cols // 2)
    per, half = p.per, p.half
    count = 2 * per
    tiles = cols // TILE
    kept = tiles - 1
    top = pl.ds(0, rows // 2)
    low = pl.ds(rows // 2, rows // 2)
    x_dev = {'col': 1 - p.col}
    y_dev = {'depth': 1 - p.depth}
    m_dev = {'row': 1 - p.row}
    engine = Engine(p, a_buf, b_buf, acc, ring, eye, a_sem, b_sem, out_sem)

    barrier = pltpu.get_barrier_semaphore()
    for dev in (x_dev, y_dev, m_dev):
        pl.semaphore_signal(barrier, inc=1, device_id=dev, device_id_type=MESH)
    pl.semaphore_wait(barrier, 3)

    def remote(src, dst, s_sem, r_sem, dev):
        return pltpu.make_async_remote_copy(src_ref=src, dst_ref=dst, send_sem=s_sem, recv_sem=r_sem, device_id=dev,
                                            device_id_type=MESH)

    def send_x(src, s, r):
        return remote(src.at[:, p.cols(r)], work.at[s, HORI, :, p.cols(r)], x_s.at[r], x_r.at[r], x_dev)

    def send_mate(src, s, r):
        return remote(src.at[:, p.cols(r)], work.at[s, MATE, :, p.cols(r)], m_s.at[r], m_r.at[r], m_dev)

    def send_y_near(src, s, q):
        return remote(src.at[:, p.cols(q)], work.at[s, VERT, :, p.cols(q)], y_s.at[q], y_r.at[q], y_dev)

    def send_y_far(src, s, q):
        far = pl.ds(p.base(1), half)
        return remote(src.at[p.rows(q), far], work.at[s, VERT, p.rows(q), far], y_s.at[per + q], y_r.at[per + q], y_dev)

    def pass_x(s, r):
        return remote(work.at[s, HORI, :, p.cols(r)], work.at[s, MATE_HORI, :, p.cols(r)], mx_s.at[r], mx_r.at[r], m_dev)

    def pass_y_near(s, q):
        return remote(work.at[s, VERT, :, p.cols(per + q)], work.at[s, MATE_VERT, :, p.cols(per + q)], my_s.at[q],
                      my_r.at[q], m_dev)

    def pass_y_far(s, q):
        near = pl.ds(p.base(0), half)
        return remote(work.at[s, VERT, p.rows(q), near], work.at[s, MATE_VERT, p.rows(q), near], my_s.at[per + q],
                      my_r.at[per + q], m_dev)

    def pass_diag(s, r):
        return remote(work.at[s, DIAG, :, p.cols(r)], work.at[s, MATE_DIAG, :, p.cols(r)], md_s.at[r], md_r.at[r], m_dev)

    def forward_x(s, r):
        return remote(work.at[s, VERT, top, p.cols(r)], work.at[s, DIAG, top, p.cols(r)], dx_s.at[r], dx_r.at[r], x_dev)

    def forward_y(s, r):
        mine = p.cols(lax.rem(r + per, count))
        return remote(work.at[s, HORI, low, mine], work.at[s, DIAG, low, mine], dy_s.at[r], dy_r.at[r], y_dev)

    def send_new(t):
        return remote(new.at[OWN], new.at[MATE], n_s.at[0], n_r.at[0], m_dev)

    def send_new_y(r):
        return remote(new.at[VERT, :, p.cols(r)], new.at[MATE_VERT, :, p.cols(r)], ny_s.at[r], ny_r.at[r], m_dev)

    def edge_x(e):
        where = p.cols(2 * kept + e)
        return remote(new.at[OWN, :, where], new.at[HORI, :, where], ex_s.at[e], ex_r.at[e], x_dev)

    def edge_y(e):
        where = p.cols(2 * kept + e - per)
        return remote(new.at[OWN, :, where], new.at[VERT, :, where], ey_s.at[e], ey_r.at[e], y_dev)

    def exchange(s, carry):
        src = work.at[s]

        @pl.when(s == 0)
        def _():
            for r in range(count):
                send_x(in_ref, 0, r).start()
                if r < per:
                    send_y_near(in_ref, 0, r).start()
                else:
                    send_y_far(in_ref, 0, r - per).start()
                send_mate(in_ref, 0, r).start()

            @pl.loop(0, tiles)
            def _(t):
                where = pl.ds(pl.multiple_of(t * TILE, TILE), TILE)
                for h, part in enumerate((top, low)):
                    load = pltpu.make_async_copy(in_ref.at[part, where], ring.at[h], out_sem.at[h, 0])
                    load.start()
                    load.wait()
                    store = pltpu.make_async_copy(ring.at[h], work.at[0, OWN, part, where], out_sem.at[h, 0])
                    store.start()
                    store.wait()

        @pl.loop(0, count)
        def _(r):
            send_mate(work.at[s, OWN], s, r).wait_recv()

        def own_load(f, q, slot):
            engine.load(src, slot, [(OWN, f * per + q), (HORI, f * per + q)],
                        [(p.right_slot(0, 0, f), q), (p.right_slot(0, 1, f), q)], 0, tiles, True)

        def near_arrive(q, slot):
            send_x(work.at[s, OWN], s, q).wait_recv()
            pass_x(s, q).start()
            own_load(0, q, slot)
            send_y_near(work.at[s, OWN], s, q).wait_recv()
            pass_y_near(s, q).start()
            pass_x(s, q).wait_recv()
            pass_y_near(s, q).wait_recv()

        def hori(tile0, nt, f, final, start, following, loaded=True):
            engine.gemm(src, per, hori_load(tile0, nt, f), 1, tile0, nt, f == 0, lambda k: [(1, f * per + k)], final,
                        start, loaded, following)

        def hori_load(tile0, nt, f):
            def load(k, slot):
                engine.load(src, slot, [(OWN, f * per + k), (HORI, f * per + k)],
                            [(p.right_slot(HORI, 0, f), k), (p.right_slot(HORI, 1, f), k)], tile0, nt, False)

            return load

        hori_final = (new.at[HORI], nothing)

        def far_prepare(q, slot):
            send_x(work.at[s, OWN], s, per + q).wait_recv()
            pass_x(s, per + q).start()
            forward_y(s, q).start()
            send_y_far(work.at[s, OWN], s, q).wait_recv()
            pass_y_far(s, q).start()

            @pl.when(q == per // 2)
            def _():
                @pl.loop(0, per)
                def _(r):
                    forward_x(s, r).start()

            @pl.when(q == per - 1)
            def _():
                @pl.loop(per, count)
                def _(r):
                    forward_x(s, r).start()
                    forward_y(s, r).start()

            pass_x(s, per + q).wait_recv()
            pass_y_far(s, q).wait_recv()
            own_load(1, q, slot)

        engine.gemm(src, per, near_arrive, 0, 0, tiles, True, lambda k: [(0, k)],
                    following=lambda slot: far_prepare(jnp.int32(0), slot))

        def far_half(q, carry):
            slot = 1 - (q // 2) % 2
            even = lax.rem(q, 2) == 0

            @pl.when(even)
            def _():
                hori_load(q, 2, 0)(0, 1 - slot)

            @pl.when(jnp.logical_not(even))
            def _():
                far_prepare(q + 1, 1 - slot)

            engine.ready(src, slot, 0, tiles, [(0, per + q)])
            engine.step(slot, 0, 0, tiles, False)

            @pl.when(even)
            def _():
                hori(q, 2, 0, None, 1 - slot, lambda after: far_prepare(q + 1, after))

            return carry

        lax.fori_loop(0, per - 1, far_half, 0)
        last = 1 - ((per - 1) // 2) % 2

        def own_before():
            vert_home(0, 1 - last)
            engine.ready(src, last, 0, tiles, [(0, count - 1)])

        def vert_home(k, slot):
            engine.load(src, slot, [(VERT, k), (VERT, per + k)], [(p.right_slot(0, 0, 0), k), (p.right_slot(0, 0, 1), k)],
                        0, kept, True)

        engine.finish(last, 0, 0, tiles, new.at[OWN], own_before, nothing)
        send_new(0).start()
        for e in range(2):
            edge_x(e).start()
            edge_y(e).start()

        def vert_away(first):
            def load(k, slot):
                r = first + 2 * k
                engine.load(src, slot, [(DIAG, r), (DIAG, r + 1)],
                            [(p.right_slot(0, 1, r // per), r % per), (p.right_slot(0, 1, (r + 1) // per), (r + 1) % per)],
                            0, kept, True)

            return load

        def diag_arrive(r, carry):
            forward_x(s, r).wait_recv()
            forward_y(s, r).wait_recv()

            @pl.when(r < 2 * kept)
            def _():
                pass_diag(s, r).start()

            return carry

        def diag_mate(r, carry):
            pass_diag(s, r).wait_recv()
            return carry

        def diag_next(first, slot):
            lax.fori_loop(first, jnp.minimum(first + 4, count), diag_arrive, 0)
            vert_away(first)(0, slot)

        engine.gemm(src, per, vert_home, 0, 0, kept, True, lambda k: [(0, k), (1, per + k)], None, 1 - last, True,
                    lambda slot: diag_next(jnp.int32(0), slot), True)

        def diag_group(g, carry):
            first = 4 * g
            slot = (last + g) % 2

            def mate_next(after):
                lax.fori_loop(first, first + 4, diag_mate, 0)
                hori_load(2 * g, 2, 1)(0, after)

            engine.gemm(src, 2, vert_away(first), 0, 0, kept, False, lambda k: [], None, slot, True, mate_next, True)
            hori(2 * g, 2, 1, hori_final, slot, lambda after: diag_next(first + 4, after))
            return carry

        lax.fori_loop(0, per // 2, diag_group, 0)

        def new_y(t):
            for e in range(2):
                send_new_y(2 * t + e).start()

        ending = (last + per // 2) % 2
        engine.finish(ending, 0, 0, kept, new.at[VERT], lambda: engine.ready(src, ending, 0, kept, []), new_y)
        send_new(0).wait_recv()

        def drain(r, carry):
            own = work.at[s, OWN]
            for copy in (send_x(own, s, r), send_mate(own, s, r), pass_x(s, r), forward_x(s, r), forward_y(s, r)):
                copy.wait_send()

            @pl.when(r < 2 * kept)
            def _():
                pass_diag(s, r).wait_send()

            @pl.when(r < per)
            def _():
                send_y_near(own, s, r).wait_send()
                send_y_far(own, s, r).wait_send()
                pass_y_near(s, r).wait_send()
                pass_y_far(s, r).wait_send()

            return carry

        lax.fori_loop(0, count, drain, 0)

        def new_y_arrive():
            def body(r, carry):
                send_new_y(r).wait_recv()
                return carry

            lax.fori_loop(0, count, body, 0)
            for e in range(2):
                edge_x(e).wait_recv()

        def all_sent():
            send_new(0).wait_send()
            for e in range(2):
                edge_x(e).wait_send()
                edge_y(e).wait_send()

            def sent(r, carry):
                send_new_y(r).wait_send()
                return carry

            lax.fori_loop(0, count, sent, 0)

        for e in range(2):
            edge_y(e).wait_recv()
            send_new_y(2 * kept + e).start()

        @pl.when(s == 0)
        def _():
            fresh = work.at[1, OWN]

            def go(t):
                for e in range(2):
                    r = 2 * t + e
                    send_x(fresh, 1, r).start()
                    send_mate(fresh, 1, r).start()

                    @pl.when(r < per)
                    def _():
                        send_y_near(fresh, 1, r).start()

            def arrive(k):
                if isinstance(k, int):
                    return

                @pl.when(k == per)
                def _():
                    new_y_arrive()

            square_tiles(engine, new, 0, 1, False, (fresh, go), arrive,
                         following=lambda slot: square_load(engine, new, 0, slot, 1, 2, False))

            def group(g, carry):
                def following(slot):
                    @pl.when(g + 1 < tiles // 2)
                    def _():
                        square_load(engine, new, 0, slot, 3 + 2 * g, 2, False)

                square_tiles(engine, new, 1 + 2 * g, 2, False, (fresh, go), loaded=True, following=following)
                return carry

            lax.fori_loop(0, tiles // 2, group, 0)
            all_sent()
            for q in range(per):
                send_y_far(fresh, 1, q).start()

        @pl.when(s > 0)
        def _():
            new_y_arrive()
            all_sent()

        return carry

    lax.fori_loop(0, SQUARINGS // 2, exchange, 0)


def last_kernel(new, out_ref, acc, a_buf, b_buf, ring, eye, a_sem, b_sem, out_sem):
    cols = out_ref.shape[1]
    p = Place(cols // 2)
    engine = Engine(p, a_buf, b_buf, acc, ring, eye, a_sem, b_sem, out_sem)
    square_tiles(engine, new, 0, cols // TILE, True, (out_ref, nothing))


def solution(mesh):
    def run(slab):
        rows, cols = slab.shape
        count = cols // SUB
        tiles = cols // TILE
        dma = pltpu.SemaphoreType.DMA
        hbm = pl.BlockSpec(memory_space=pl.ANY)

        def scratch(n_acc):
            return [
                pltpu.VMEM((n_acc, tiles, rows, TILE), jnp.float32),
                pltpu.VMEM((2, rows, 2 * SUB), jnp.bfloat16),
                pltpu.VMEM((2, 2 * SUB, cols), jnp.bfloat16),
                pltpu.VMEM((RING, rows // 2, TILE), jnp.bfloat16),
                pltpu.VMEM((SUB, SUB), jnp.bfloat16),
                dma((2,)), dma((2,)), dma((RING, 2)),
            ]

        new, _ = pl.pallas_call(
            pair_kernel,
            out_shape=(jax.ShapeDtypeStruct((5, rows, cols), jnp.bfloat16),
                       jax.ShapeDtypeStruct((2, 8, rows, cols), jnp.bfloat16)),
            in_specs=[hbm],
            out_specs=(hbm, hbm),
            scratch_shapes=scratch(2) + [dma((count,)) for _ in range(16)] + [dma((1,)), dma((1,)), dma((count,)),
                                                                              dma((count,))] + [dma((2,))] * 4,
            compiler_params=pltpu.CompilerParams(collective_id=0, has_side_effects=True, vmem_limit_bytes=67_000_000),
            name='reach_pairs',
        )(slab)
        return pl.pallas_call(
            last_kernel,
            out_shape=jax.ShapeDtypeStruct((rows, cols), jnp.bfloat16),
            in_specs=[hbm],
            out_specs=hbm,
            scratch_shapes=scratch(1),
            compiler_params=pltpu.CompilerParams(vmem_limit_bytes=67_000_000),
            name='reach_last',
        )(new)

    layout = P(('row', 'depth'), 'col')
    return jax.shard_map(run, mesh=mesh, in_specs=(layout,), out_specs=layout, check_vma=False)
```
